256 devices in a mesh: expert: 8 (over y_lo, x), rep: 32 (over z, y_hi, core).
Axes of the slice: x: 4, y: 4 (y_hi: 2, y_lo: 2; y = y_hi * 2 + y_lo), z: 8, core: 2. Of those that a mesh axis runs over, the one named last changes fastest.
Arguments:
- route_ids: int32 [2048, 2], P(('expert', 'rep')), may hold values from 0 to 7, all different within a row; in each aligned block of 8 rows (0 to 7, 8 to 15, ...) at most 4 rows name the same one
- route_weight: float32 [2048, 2], P(('expert', 'rep')), may hold values from 0.2 to 0.8
- input_float: bfloat16 [2048, 4096], P(('expert', 'rep')), may hold values from -6 to 6
- input_quant: bfloat16 [2048, 4096], P(('expert', 'rep')), may hold values from -6 to 6
- keep_mask: int32 [2048, 4096], P(('expert', 'rep')), may hold values 0 or 1
- grad_mixed: bfloat16 [2048, 4096], P(('expert', 'rep')), may hold values from -192 to 192
- gate_weight: bfloat16 [8, 4096, 7168], P('expert', None, 'rep'), may hold values from -0.09375 to 0.09375
- up_weight: bfloat16 [8, 4096, 7168], P('expert', None, 'rep'), may hold values from -0.09375 to 0.09375
- down_base: bfloat16 [8, 7168, 4096], P('expert', 'rep'), may hold values from -0.0625 to 0.0625
- down_round: bfloat16 [8, 7168, 4096], P('expert', 'rep'), may hold values from -8 to 8
- down_step: float32 [8, 4096], P('expert'), may hold values from 0.004 to 0.04
Outputs:
- mixed: bfloat16 [2048, 4096], P(('expert', 'rep'))
- round_grad: float32 [8, 7168, 4096], P('expert', 'rep')
The draws below stay inside these ranges and needn't reach their ends.
Inputs may be any that keep to these rules, and one draw needn't show every extreme that they name: `route_ids`: within the 8 tokens of one device, each expert is named by at most 4 pairs; the two experts of a token differ.
All inputs are finite; a program needn't handle non-finite values. No bound on the sum of `keep_mask` on one device may be relied on, other than what follows from the above.
Results may differ from the reference program's by a relative error of at most 0.0065.
Values may be sent and summed in bfloat16 or wider, within the bound.
No kernel may reach another device: no remote copies, remote signals or barrier semaphores. Data moves between devices by JAX's collectives and lax.ppermute only.
A program may use at most 128 MiB of HBM per device.

```python
import math
import jax
import jax.numpy as jnp
import numpy as np
from jax import lax

D = 4096
FF = 7168
TOK_DEV = 8
CAP = 4
EXPERTS = 8
TOKENS = 2048


def touch_ends(result, rng, low, top_value):
    index_at = [jax.random.randint(jax.random.fold_in(rng, axis), (), 0, length) for axis, length in enumerate(result.shape)]
    main_axis = result.shape.index(max(result.shape))
    neighbour = index_at[:main_axis] + [(index_at[main_axis] + 1) % result.shape[main_axis]] + index_at[main_axis + 1:]
    return result.at[tuple(index_at)].set(low).at[tuple(neighbour)].set(top_value)


def shard_levels(stream_key, shape, split, low, top_value):
    loudness = 1.0
    for dim, shards_of in split:
        draws = jax.random.uniform(jax.random.fold_in(jax.random.fold_in(stream_key, 6), dim), (shards_of,), jnp.float32, low / len(split), top_value / len(split))
        loudness = loudness * jnp.repeat(jnp.exp(draws), shape[dim] // shards_of).reshape((-1,) + (1,) * (len(shape) - 1 - dim))
    return loudness


def assign_block(own_key, own, number, rows, count, top, limit, slope):
    ranking = jax.random.permutation(own_key, count)
    heavy_load, ordinary = portions_of(count, rows * top, limit, slope, True), portions_of(count, rows * top, limit, slope, False)
    places = jnp.arange(count)

    def named(sizes, offset_by):
        used = int((sizes > 0).sum())
        fixed = max(1, used // 4)
        moved = fixed + (places - fixed + offset_by * (used - fixed)) % max(1, count - fixed)
        return jnp.zeros((count,), jnp.int32).at[ranking[jnp.where(places < fixed, places, moved)]].set(jnp.asarray(sizes, jnp.int32))

    sizes = jnp.where(number % 4 == 0, named(heavy_load, number // 4), named(ordinary, number - number // 4 - 1))
    mixed = jax.random.permutation(jax.random.fold_in(own, 3), count)
    donor, sink = mixed[0:count // 2 * 2:2], mixed[1:count // 2 * 2:2]
    room = jnp.minimum(sizes[donor] - 1, limit - sizes[sink]) // 2
    room = jnp.where((donor == ranking[0]) | (sink == ranking[0]) | (sizes[sink] == 0), 0, jnp.maximum(room, 0))
    moved = jax.random.randint(jax.random.fold_in(own, 4), (count // 2,), 0, 1 << 20) % (room + 1)
    sizes = sizes.at[donor].add(-moved).at[sink].add(moved)
    items = jnp.searchsorted(jnp.cumsum(sizes), jnp.arange(rows * top), side="right").astype(jnp.int32)
    grid = items.reshape(top, rows).T
    grid = grid[jax.random.permutation(jax.random.fold_in(own, 1), rows)]
    offset_by = jax.random.randint(jax.random.fold_in(own, 2), (rows, 1), 0, top)
    return jnp.take_along_axis(grid, (jnp.arange(top)[None, :] + offset_by) % top, axis=1)


def portions_of(count, total, bound, skew, full):
    weights = [(1 << 20) // math.isqrt(standing ** skew) + 1 for standing in range(1, count + 1)]
    largest = bound if full else min(bound, max(-(-total // count), total * weights[0] // sum(weights)))
    least = 1 if total - largest >= count - 1 else 0
    counts, surplus = [largest] + [least] * (count - 1), total - largest - least * (count - 1)
    while surplus > 0:
        free = [i for i in range(1, count) if counts[i] < largest] or [i for i in range(1, count) if counts[i] < bound]
        mass, remaining = sum([weights[i] for i in free]), surplus
        for i in free:
            more = min(bound - counts[i], max(1, remaining * weights[i] // mass), surplus)
            counts[i] = counts[i] + more
            surplus = surplus - more
    return np.array(counts)


def bell_draw(key, dims, scale, reach, pieces=(), kind=jnp.bfloat16):
    factor_of = shard_levels(key, dims, pieces, -0.22, 0.18) if pieces else 1.0
    array = jax.random.normal(key, dims, jnp.float32) * scale * factor_of
    return jnp.minimum(jnp.maximum(array, -reach), reach).astype(kind)


def setup_inputs(seed: int = 0) -> dict:
    arg_keys = jax.random.split(jax.random.key(seed), 12)
    route_ids_keys = jax.random.split(jax.random.fold_in(arg_keys[0], 1), TOKENS // TOK_DEV)
    route_ids_turns = jax.random.permutation(jax.random.fold_in(arg_keys[0], 3), TOKENS // TOK_DEV)
    route_ids = jax.vmap(lambda own, number: assign_block(jax.random.fold_in(arg_keys[0], 2), own, number, TOK_DEV, EXPERTS, 2, CAP, 2))(route_ids_keys, route_ids_turns).reshape((TOKENS, 2))
    route_weight = jnp.clip(0.2 + 0.6 * jax.random.uniform(arg_keys[1], (TOKENS, 2), jnp.float32) ** shard_levels(arg_keys[1], (TOKENS, 2), ((0, 256),), -0.2, 0.2), 0.2, 0.8)
    input_float = bell_draw(arg_keys[2], (TOKENS, D), 1.0, 6.0, ((0, 256),))
    input_quant = bell_draw(arg_keys[3], (TOKENS, D), 1.0, 6.0, ((0, 256),))
    keep_mask = touch_ends((jax.random.randint(arg_keys[4], (TOKENS, D), 0, 2) < 1).astype(jnp.int32), jax.random.fold_in(arg_keys[4], 1), 0, 1)
    grad_mixed = bell_draw(arg_keys[5], (TOKENS, D), 32.0, 192.0, ((0, 256),))
    gate_weight = bell_draw(arg_keys[6], (EXPERTS, D, FF), D ** -0.5, 0.09375, ((0, 8), (2, 32)))
    up_weight = bell_draw(arg_keys[7], (EXPERTS, D, FF), D ** -0.5, 0.09375, ((0, 8), (2, 32)))
    down_base = bell_draw(arg_keys[8], (EXPERTS, FF, D), FF ** -0.5, 0.0625, ((0, 8), (1, 32)))
    down_round = bell_draw(arg_keys[9], (EXPERTS, FF, D), 2.0, 8.0, ((0, 8), (1, 32)))
    down_step = jnp.clip(jnp.exp(math.log(0.04) - 2.30258502 * jax.random.uniform(arg_keys[10], (EXPERTS, D), jnp.float32) ** shard_levels(arg_keys[10], (EXPERTS, D), ((0, 8),), -0.2, 0.2)), 0.004, 0.04)
    return dict(route_ids=route_ids, route_weight=route_weight, input_float=input_float, input_quant=input_quant, keep_mask=keep_mask, grad_mixed=grad_mixed, gate_weight=gate_weight, up_weight=up_weight, down_base=down_base, down_round=down_round, down_step=down_step)


def slots_of(route_ids):
    groups = route_ids.shape[0] // TOK_DEV
    flat = route_ids.reshape(groups, TOK_DEV * 2)
    onehot = (flat[:, :, None] == jnp.arange(EXPERTS, dtype=jnp.int32)[None, None, :]).astype(jnp.int32)
    before = jnp.cumsum(onehot, axis=1) - onehot
    return jnp.sum(before * onehot, axis=2).reshape(route_ids.shape[0], 2).astype(jnp.int32)


def reference(route_ids, route_weight, input_float, input_quant, keep_mask, grad_mixed, gate_weight, up_weight, down_base, down_round, down_step):
    tokens = route_ids.shape[0]
    groups = tokens // TOK_DEV
    slot = slots_of(route_ids)
    x_in = jnp.where(keep_mask == 1, input_quant, input_float)
    group = (jnp.arange(tokens, dtype=jnp.int32) // TOK_DEV).astype(jnp.int32)
    position = (group[:, None] * CAP + slot).astype(jnp.int32)
    x_pair = jnp.broadcast_to(x_in[:, None, :], (tokens, 2, D))
    rows = jnp.zeros((EXPERTS, groups * CAP, D), jnp.bfloat16).at[route_ids, position].set(x_pair)
    weighted = (route_weight[:, :, None] * grad_mixed.astype(jnp.float32)[:, None, :]).astype(jnp.bfloat16)
    cot = jnp.zeros((EXPERTS, groups * CAP, D), jnp.bfloat16).at[route_ids, position].set(weighted)

    def one_expert(items):
        rows_e, cot_e, gate_e, up_e, base_e, round_e, step_e = items
        gate = jnp.dot(rows_e, gate_e, preferred_element_type=jnp.float32)
        up = jnp.dot(rows_e, up_e, preferred_element_type=jnp.float32)
        hidden = (jax.nn.silu(gate) * up).astype(jnp.bfloat16)
        soft = jax.nn.sigmoid(round_e.astype(jnp.float32))
        quant = (base_e.astype(jnp.float32) + step_e[None, :] * soft).astype(jnp.bfloat16)
        out = jnp.dot(hidden, quant, preferred_element_type=jnp.float32).astype(jnp.bfloat16)
        grad_w = lax.dot_general(hidden, cot_e, (((0,), (0,)), ((), ())), preferred_element_type=jnp.float32)
        return out, grad_w * step_e[None, :] * soft * (1.0 - soft)

    expert_out, round_grad = lax.map(one_expert, (rows, cot, gate_weight, up_weight, down_base, down_round, down_step))
    picked = expert_out[route_ids, position].astype(jnp.float32)
    mixed = jnp.sum(route_weight[:, :, None] * picked, axis=1).astype(jnp.bfloat16)
    return mixed, round_grad
```

```python
import jax
import jax.numpy as jnp
from jax import lax
from jax.sharding import PartitionSpec as P


def local_slots(route_ids, experts):
    count = route_ids.shape[0]
    flat = route_ids.reshape(count * 2)
    onehot = (flat[:, None] == jnp.arange(experts, dtype=jnp.int32)[None, :]).astype(jnp.int32)
    before = jnp.cumsum(onehot, axis=0) - onehot
    return jnp.sum(before * onehot, axis=1).reshape(count, 2)


def swap(a, bit):
    n = lax.axis_size("rep")
    return lax.ppermute(a, "rep", [(r, r ^ bit) for r in range(n)])


def along_z(a, sign):
    n = lax.axis_size("rep")
    return lax.ppermute(a, "rep", [(r, (r + 4 * sign) % n) for r in range(n)])


def gather_ring(rows, far):
    rings = lax.axis_size("rep") // 4
    half = rings // 2
    held = {0: rows}
    for sign in (1, -1):
        block = rows
        for step in range(1, half + (1 if sign == far else 0)):
            block = along_z(block, sign)
            held[(-sign * step) % rings] = block
    return held


def reduce_ring(parts, far):
    rings = lax.axis_size("rep") // 4
    half = rings // 2
    total = parts[0]
    for sign in (1, -1):
        count = half if sign == far else half - 1
        message = parts[(sign * count) % rings].astype(jnp.bfloat16)
        for step in range(count - 1, -1, -1):
            came = along_z(message, sign).astype(jnp.float32)
            if step:
                message = (parts[(sign * step) % rings] + came).astype(jnp.bfloat16)
            else:
                total = total + came
    return total


def body(
    route_ids,
    route_weight,
    input_float,
    input_quant,
    keep_mask,
    grad_mixed,
    gate_weight,
    up_weight,
    down_base,
    down_round,
    down_step,
):
    experts = lax.axis_size("expert")
    rings = lax.axis_size("rep") // 4
    here = lax.axis_index("rep")
    at_core, at_y, at_z = (here % 2, here // 2 % 2, here // 4)
    count = route_ids.shape[0]
    capacity = count // 2
    slot = local_slots(route_ids, experts)
    target = route_ids * capacity + slot
    columns = jnp.arange(experts * capacity, dtype=jnp.int32)
    first = (target[:, 0:1] == columns[None, :]).astype(jnp.float32)
    second = (target[:, 1:2] == columns[None, :]).astype(jnp.float32)
    placing = (first + second).astype(jnp.bfloat16)
    weighting = route_weight[:, 0:1] * first + route_weight[:, 1:2] * second
    x_in = jnp.where(keep_mask == 1, input_quant, input_float)
    send_rows = lax.dot_general(
        placing, x_in, (((0,), (0,)), ((), ())), preferred_element_type=jnp.float32
    ).astype(jnp.bfloat16)
    send_cot = lax.dot_general(
        weighting,
        grad_mixed.astype(jnp.float32),
        (((0,), (0,)), ((), ())),
        precision=lax.Precision.HIGHEST,
        preferred_element_type=jnp.float32,
    ).astype(jnp.bfloat16)
    own_rows = lax.all_to_all(send_rows, "expert", split_axis=0, concat_axis=0, tiled=True)
    own_cot = lax.all_to_all(send_cot, "expert", split_axis=0, concat_axis=0, tiled=True)
    all_cot = lax.all_gather(own_cot, "rep", axis=0, tiled=True)
    units = gate_weight.shape[2]
    w_gate = jnp.swapaxes(gate_weight[0], 0, 1)
    w_up = jnp.swapaxes(up_weight[0], 0, 1)
    soft = jax.nn.sigmoid(down_round[0].astype(jnp.float32))
    step_row = down_step[0][None, :]
    quant_down = (down_base[0].astype(jnp.float32) + step_row * soft).astype(jnp.bfloat16)
    w_gate = jnp.concatenate([w_gate, swap(w_gate, 1)], axis=0)
    w_up = jnp.concatenate([w_up, swap(w_up, 1)], axis=0)
    quant_down = jnp.concatenate([quant_down, swap(quant_down, 1)], axis=0)
    size = own_rows.shape[0]
    mine = gather_ring(own_rows, 1)
    theirs = gather_ring(swap(own_rows, 2), -1)

    def hidden_of(which):
        x = jnp.concatenate([b[k] for k in which for b in (mine, theirs)], axis=0)
        dims = (((1,), (1,)), ((), ()))
        gate = lax.dot_general(x, w_gate, dims, preferred_element_type=jnp.float32)
        up = lax.dot_general(x, w_up, dims, preferred_element_type=jnp.float32)
        return (jax.nn.silu(gate) * up).astype(jnp.bfloat16)

    half = rings // 2
    near = [k % rings for k in range(-(half - 2), half - 1)]
    away = [k % rings for k in (half - 1, half, half + 1)]
    hidden, part = ({}, {})
    for which in (away, near):
        block = hidden_of(which)
        out = jnp.dot(block, quant_down, preferred_element_type=jnp.float32)
        for i, k in enumerate(which):
            hidden[k] = block[2 * size * i : 2 * size * (i + 1)]
            part[k] = out[2 * size * i : 2 * size * (i + 1)]
    for_other = reduce_ring({k: v[size:] for k, v in part.items()}, -1)
    for_me = reduce_ring({k: v[:size] for k, v in part.items()}, 1)
    came = swap(for_other.astype(jnp.bfloat16), 2)
    summed = (for_me + came.astype(jnp.float32)).astype(jnp.bfloat16)
    returned = lax.all_to_all(summed, "expert", split_axis=0, concat_axis=0, tiled=True)
    mixed = jnp.dot(
        weighting,
        returned.astype(jnp.float32),
        precision=lax.Precision.HIGHEST,
        preferred_element_type=jnp.float32,
    ).astype(jnp.bfloat16)
    both = jnp.stack([hidden[k] for k in range(rings)]).reshape(rings, 2, size, 2 * units)
    twice = jnp.concatenate([both, both], axis=0)
    placed = lax.dynamic_slice_in_dim(twice, (rings - at_z) % rings, rings, axis=0)
    placed = jnp.where(at_y == 1, placed[:, ::-1], placed)
    ours, other = (placed[..., :units], swap(placed[..., units:], 1))
    full = jnp.where(
        at_core == 0, jnp.stack([ours, other], axis=2), jnp.stack([other, ours], axis=2)
    ).reshape(4 * rings * size, units)
    grad_w = lax.dot_general(
        full, all_cot, (((0,), (0,)), ((), ())), preferred_element_type=jnp.float32
    )
    round_grad = (grad_w * step_row * soft * (1.0 - soft))[None]
    return (mixed, round_grad)


def solution(mesh):
    return jax.shard_map(
        body,
        mesh=mesh,
        in_specs=(
            P(("expert", "rep"), None),
            P(("expert", "rep"), None),
            P(("expert", "rep"), None),
            P(("expert", "rep"), None),
            P(("expert", "rep"), None),
            P(("expert", "rep"), None),
            P("expert", None, "rep"),
            P("expert", None, "rep"),
            P("expert", "rep", None),
            P("expert", "rep", None),
            P("expert", None),
        ),
        out_specs=(P(("expert", "rep"), None), P("expert", "rep", None)),
        check_vma=False,
    )
```

```python
import jax
import jax.numpy as jnp
from jax import lax
from jax.sharding import PartitionSpec as P


BOTH = ("expert", "rep")


def swap_cores(a):
    n = lax.axis_size("rep")
    return lax.ppermute(a, "rep", [(r, r ^ 1) for r in range(n)])


def along_z(a, sign):
    n = lax.axis_size("rep")
    return lax.ppermute(a, "rep", [(r, (r + 4 * sign) % n) for r in range(n)])


def exchange(a):
    experts, n = (lax.axis_size("expert"), lax.axis_size("rep"))
    groups = [
        [e * n + 4 * z + 2 * y + c for y in range(2) for e in range(experts)]
        for z in range(n // 4)
        for c in range(2)
    ]
    return lax.all_to_all(
        a, BOTH, split_axis=0, concat_axis=0, tiled=True, axis_index_groups=groups
    )


def gather_ring(rows):
    rings = lax.axis_size("rep") // 4
    half = rings // 2
    cut = rows.shape[0] // 2
    held = {0: rows}
    up = down = rows
    for step in range(1, half):
        up, down = (along_z(up, 1), along_z(down, -1))
        held[rings - step], held[step] = (up, down)
    held[half] = jnp.concatenate([along_z(up[:cut], 1), along_z(down[cut:], -1)], axis=0)
    return held


def reduce_ring(parts):
    rings = lax.axis_size("rep") // 4
    half = rings // 2
    cut = parts[0].shape[0] // 2
    up = along_z(parts[half][:cut].astype(jnp.bfloat16), 1).astype(jnp.float32)
    down = along_z(parts[half][cut:].astype(jnp.bfloat16), -1).astype(jnp.float32)
    up = jnp.concatenate([up, jnp.zeros_like(down)], axis=0)
    down = jnp.concatenate([jnp.zeros_like(up[:cut]), down], axis=0)
    for step in range(half - 1, 0, -1):
        up = along_z((parts[step] + up).astype(jnp.bfloat16), 1).astype(jnp.float32)
        down = along_z((parts[rings - step] + down).astype(jnp.bfloat16), -1).astype(jnp.float32)
    return parts[0] + up + down


def local_slots(route_ids, experts):
    count = route_ids.shape[0]
    flat = route_ids.reshape(count * 2)
    onehot = (flat[:, None] == jnp.arange(experts, dtype=jnp.int32)[None, :]).astype(jnp.int32)
    before = jnp.cumsum(onehot, axis=0) - onehot
    return jnp.sum(before * onehot, axis=1).reshape(count, 2)


def body(
    route_ids,
    route_weight,
    input_float,
    input_quant,
    keep_mask,
    grad_mixed,
    gate_weight,
    up_weight,
    down_base,
    down_round,
    down_step,
):
    experts = lax.axis_size("expert")
    rings = lax.axis_size("rep") // 4
    here = lax.axis_index("rep")
    at_core, at_z = (here & 1, here >> 2)
    count = route_ids.shape[0]
    capacity = count // 2
    slot = local_slots(route_ids, experts)
    target = route_ids * capacity + slot
    columns = jnp.arange(experts * capacity, dtype=jnp.int32)
    first = (target[:, 0:1] == columns[None, :]).astype(jnp.float32)
    second = (target[:, 1:2] == columns[None, :]).astype(jnp.float32)
    placing = (first + second).astype(jnp.bfloat16)
    weighting = route_weight[:, 0:1] * first + route_weight[:, 1:2] * second
    x_in = jnp.where(keep_mask == 1, input_quant, input_float)
    send_cot = lax.dot_general(
        weighting,
        grad_mixed.astype(jnp.float32),
        (((0,), (0,)), ((), ())),
        precision=lax.Precision.HIGHEST,
        preferred_element_type=jnp.float32,
    ).astype(jnp.bfloat16)
    own_cot = lax.all_to_all(send_cot, "expert", split_axis=0, concat_axis=0, tiled=True)
    send_rows = lax.dot_general(
        jnp.concatenate([placing, placing], axis=1),
        x_in,
        (((0,), (0,)), ((), ())),
        preferred_element_type=jnp.float32,
    ).astype(jnp.bfloat16)
    own_rows = exchange(send_rows)
    all_cot = lax.all_gather(own_cot, "rep", axis=0, tiled=True)
    units = gate_weight.shape[2]
    w_gate = jnp.swapaxes(gate_weight[0], 0, 1)
    w_up = jnp.swapaxes(up_weight[0], 0, 1)
    soft = jax.nn.sigmoid(down_round[0].astype(jnp.float32))
    step_row = down_step[0][None, :]
    quant_down = (down_base[0].astype(jnp.float32) + step_row * soft).astype(jnp.bfloat16)
    w_gate = jnp.concatenate([w_gate, swap_cores(w_gate)], axis=0)
    w_up = jnp.concatenate([w_up, swap_cores(w_up)], axis=0)
    quant_down = jnp.concatenate([quant_down, swap_cores(quant_down)], axis=0)
    size = own_rows.shape[0]
    held = gather_ring(own_rows)

    def hidden_of(which):
        x = jnp.concatenate([held[k] for k in which], axis=0)
        dims = (((1,), (1,)), ((), ()))
        gate = lax.dot_general(x, w_gate, dims, preferred_element_type=jnp.float32)
        up = lax.dot_general(x, w_up, dims, preferred_element_type=jnp.float32)
        return (jax.nn.silu(gate) * up).astype(jnp.bfloat16)

    half = rings // 2
    near = [k % rings for k in range(-(half - 2), half - 1)]
    away = [half - 1, half, half + 1]
    hidden, part = ({}, {})
    for which in (away, near):
        block = hidden_of(which)
        out = jnp.dot(block, quant_down, preferred_element_type=jnp.float32)
        for i, k in enumerate(which):
            hidden[k] = block[size * i : size * (i + 1)]
            part[k] = out[size * i : size * (i + 1)]
    summed = reduce_ring(part).astype(jnp.bfloat16)
    summed, all_cot = lax.optimization_barrier((summed, all_cot))
    returned = exchange(summed)
    mixed = jnp.dot(
        jnp.concatenate([weighting, weighting], axis=1),
        returned.astype(jnp.float32),
        precision=lax.Precision.HIGHEST,
        preferred_element_type=jnp.float32,
    ).astype(jnp.bfloat16)
    both = jnp.stack([hidden[k] for k in range(rings)]).reshape(rings, 2, size // 2, 2 * units)
    twice = jnp.concatenate([both, both], axis=0)
    placed = lax.dynamic_slice_in_dim(twice, (rings - at_z) & (rings - 1), rings, axis=0)
    ours, other = (placed[..., :units], swap_cores(placed[..., units:]))
    full = jnp.where(
        at_core == 0, jnp.stack([ours, other], axis=2), jnp.stack([other, ours], axis=2)
    ).reshape(2 * rings * size, units)
    grad_w = lax.dot_general(
        full, all_cot, (((0,), (0,)), ((), ())), preferred_element_type=jnp.float32
    )
    round_grad = (grad_w * step_row * soft * (1.0 - soft))[None]
    return (mixed, round_grad)


def solution(mesh):
    return jax.shard_map(
        body,
        mesh=mesh,
        in_specs=(
            P(("expert", "rep"), None),
            P(("expert", "rep"), None),
            P(("expert", "rep"), None),
            P(("expert", "rep"), None),
            P(("expert", "rep"), None),
            P(("expert", "rep"), None),
            P("expert", None, "rep"),
            P("expert", None, "rep"),
            P("expert", "rep", None),
            P("expert", "rep", None),
            P("expert", None),
        ),
        out_specs=(P(("expert", "rep"), None), P("expert", "rep", None)),
        check_vma=False,
    )
```

```python
import jax
import jax.numpy as jnp
from jax import lax
from jax.sharding import PartitionSpec as P


BOTH = ("expert", "rep")


def swap_cores(a):
    n = lax.axis_size("rep")
    return lax.ppermute(a, "rep", [(r, r ^ 1) for r in range(n)])


def along_z(a, sign):
    n = lax.axis_size("rep")
    return lax.ppermute(a, "rep", [(r, (r + 4 * sign) % n) for r in range(n)])


def exchange(a):
    experts, n = (lax.axis_size("expert"), lax.axis_size("rep"))
    groups = [
        [e * n + 4 * z + 2 * y + c for y in range(2) for e in range(experts)]
        for z in range(n // 4)
        for c in range(2)
    ]
    return lax.all_to_all(
        a, BOTH, split_axis=0, concat_axis=0, tiled=True, axis_index_groups=groups
    )


def gather_ring(rows):
    rings = lax.axis_size("rep") // 4
    half = rings // 2
    cut = rows.shape[0] // 2
    held = {0: rows}
    up = down = rows
    for step in range(1, half):
        up, down = lax.optimization_barrier((along_z(up, 1), along_z(down, -1)))
        held[rings - step], held[step] = (up, down)
    held[half] = jnp.concatenate([along_z(up[:cut], 1), along_z(down[cut:], -1)], axis=0)
    return held


def reduce_ring(parts):
    rings = lax.axis_size("rep") // 4
    half = rings // 2
    cut = parts[0].shape[0] // 2
    far = parts[half].astype(jnp.bfloat16)
    up, down = lax.optimization_barrier((along_z(far[:cut], 1), along_z(far[cut:], -1)))
    up = jnp.concatenate([up, jnp.zeros_like(down)], axis=0)
    down = jnp.concatenate([jnp.zeros_like(up[:cut]), down], axis=0)
    for step in range(half - 1, 0, -1):
        up = (parts[step] + up.astype(jnp.float32)).astype(jnp.bfloat16)
        down = (parts[rings - step] + down.astype(jnp.float32)).astype(jnp.bfloat16)
        up, down = lax.optimization_barrier((along_z(up, 1), along_z(down, -1)))
    return parts[0] + up.astype(jnp.float32) + down.astype(jnp.float32)


def local_slots(route_ids, experts):
    count = route_ids.shape[0]
    flat = route_ids.reshape(count * 2)
    onehot = (flat[:, None] == jnp.arange(experts, dtype=jnp.int32)[None, :]).astype(jnp.int32)
    before = jnp.cumsum(onehot, axis=0) - onehot
    return jnp.sum(before * onehot, axis=1).reshape(count, 2)


def body(
    route_ids,
    route_weight,
    input_float,
    input_quant,
    keep_mask,
    grad_mixed,
    gate_weight,
    up_weight,
    down_base,
    down_round,
    down_step,
):
    experts = lax.axis_size("expert")
    rings = lax.axis_size("rep") // 4
    here = lax.axis_index("rep")
    at_core, at_z = (here & 1, here >> 2)
    count = route_ids.shape[0]
    capacity = count // 2
    slot = local_slots(route_ids, experts)
    target = route_ids * capacity + slot
    columns = jnp.arange(experts * capacity, dtype=jnp.int32)
    first = (target[:, 0:1] == columns[None, :]).astype(jnp.float32)
    second = (target[:, 1:2] == columns[None, :]).astype(jnp.float32)
    placing = (first + second).astype(jnp.bfloat16)
    weighting = route_weight[:, 0:1] * first + route_weight[:, 1:2] * second
    x_in = jnp.where(keep_mask == 1, input_quant, input_float)
    send_cot = lax.dot_general(
        weighting,
        grad_mixed.astype(jnp.float32),
        (((0,), (0,)), ((), ())),
        precision=lax.Precision.HIGHEST,
        preferred_element_type=jnp.float32,
    ).astype(jnp.bfloat16)
    send_rows = lax.dot_general(
        jnp.concatenate([placing, placing], axis=1),
        x_in,
        (((0,), (0,)), ((), ())),
        preferred_element_type=jnp.float32,
    ).astype(jnp.bfloat16)
    own_rows, send_cot = lax.optimization_barrier((exchange(send_rows), send_cot))
    own_cot = lax.all_to_all(send_cot, "expert", split_axis=0, concat_axis=0, tiled=True)
    all_cot = lax.all_gather(own_cot, "rep", axis=0, tiled=True)
    units = gate_weight.shape[2]
    w_gate = jnp.swapaxes(gate_weight[0], 0, 1)
    w_up = jnp.swapaxes(up_weight[0], 0, 1)
    soft = jax.nn.sigmoid(down_round[0].astype(jnp.float32))
    step_row = down_step[0][None, :]
    quant_down = (down_base[0].astype(jnp.float32) + step_row * soft).astype(jnp.bfloat16)
    quant_down, slope = lax.optimization_barrier((quant_down, step_row * soft * (1.0 - soft)))
    w_gate = jnp.concatenate([w_gate, swap_cores(w_gate)], axis=0)
    w_up = jnp.concatenate([w_up, swap_cores(w_up)], axis=0)
    quant_down = jnp.concatenate([quant_down, swap_cores(quant_down)], axis=0)
    size = own_rows.shape[0]
    held = gather_ring(own_rows)

    def hidden_of(which):
        x = jnp.concatenate([held[k] for k in which], axis=0)
        dims = (((1,), (1,)), ((), ()))
        gate = lax.dot_general(x, w_gate, dims, preferred_element_type=jnp.float32)
        up = lax.dot_general(x, w_up, dims, preferred_element_type=jnp.float32)
        return (jax.nn.silu(gate) * up).astype(jnp.bfloat16)

    half = rings // 2
    near = [k % rings for k in range(-(half - 2), half - 1)]
    hidden, part = ({}, {})
    for which in ([half, half - 1, half + 1], near):
        block = hidden_of(which)
        for i, k in enumerate(which):
            hidden[k] = block[size * i : size * (i + 1)]
    for which in ([half], near + [half - 1, half + 1]):
        block = jnp.concatenate([hidden[k] for k in which], axis=0)
        out = jnp.dot(block, quant_down, preferred_element_type=jnp.float32)
        for i, k in enumerate(which):
            part[k] = out[size * i : size * (i + 1)]
    summed = reduce_ring(part).astype(jnp.bfloat16)
    summed, all_cot = lax.optimization_barrier((summed, all_cot))
    returned = exchange(summed)
    mixed = jnp.dot(
        jnp.concatenate([weighting, weighting], axis=1),
        returned.astype(jnp.float32),
        precision=lax.Precision.HIGHEST,
        preferred_element_type=jnp.float32,
    ).astype(jnp.bfloat16)
    placed = jnp.zeros((rings, 2, size // 2, 2 * units), jnp.bfloat16)
    for k in range(rings):
        block = hidden[k].reshape(1, 2, size // 2, 2 * units)
        placed = lax.dynamic_update_slice_in_dim(placed, block, (at_z + k) & (rings - 1), axis=0)
    ours, other = (placed[..., :units], swap_cores(placed[..., units:]))
    full = jnp.where(
        at_core == 0, jnp.stack([ours, other], axis=2), jnp.stack([other, ours], axis=2)
    ).reshape(2 * rings * size, units)
    grad_w = lax.dot_general(
        full, all_cot, (((0,), (0,)), ((), ())), preferred_element_type=jnp.float32
    )
    round_grad = (grad_w * slope)[None]
    return (mixed, round_grad)


def solution(mesh):
    return jax.shard_map(
        body,
        mesh=mesh,
        in_specs=(
            P(("expert", "rep"), None),
            P(("expert", "rep"), None),
            P(("expert", "rep"), None),
            P(("expert", "rep"), None),
            P(("expert", "rep"), None),
            P(("expert", "rep"), None),
            P("expert", None, "rep"),
            P("expert", None, "rep"),
            P("expert", "rep", None),
            P("expert", "rep", None),
            P("expert", None),
        ),
        out_specs=(P(("expert", "rep"), None), P("expert", "rep", None)),
        check_vma=False,
    )
```

```python
import jax
import jax.numpy as jnp
from jax import lax
from jax.sharding import PartitionSpec as P


BOTH = ("expert", "rep")


def swap_cores(a):
    n = lax.axis_size("rep")
    return lax.ppermute(a, "rep", [(r, r ^ 1) for r in range(n)])


def along_z(a, sign, name):
    n = lax.axis_size("rep")
    with jax.named_scope(name + ("_up" if sign > 0 else "_down")):
        return lax.ppermute(a, "rep", [(r, (r + 4 * sign) % n) for r in range(n)])


def exchange(a):
    experts, n = (lax.axis_size("expert"), lax.axis_size("rep"))
    groups = [
        [e * n + 4 * z + 2 * y + c for y in range(2) for e in range(experts)]
        for z in range(n // 4)
        for c in range(2)
    ]
    return lax.all_to_all(
        a, BOTH, split_axis=0, concat_axis=0, tiled=True, axis_index_groups=groups
    )


def gather_tokens(a):
    experts, n = (lax.axis_size("expert"), lax.axis_size("rep"))
    order = [
        e * n + 4 * z + 2 * y + c
        for z in range(n // 4)
        for y in range(2)
        for e in range(experts)
        for c in range(2)
    ]
    return lax.all_gather(a, BOTH, axis=0, tiled=True, axis_index_groups=[order])


def gather_ring(rows):
    rings = lax.axis_size("rep") // 4
    half = rings // 2
    cut = rows.shape[0] // 2
    held = {0: rows}
    up = down = rows
    for step in range(1, half):
        up, down = lax.optimization_barrier(
            (along_z(up, 1, f"gather{step}"), along_z(down, -1, f"gather{step}"))
        )
        held[rings - step], held[step] = (up, down)
    held[half] = jnp.concatenate(
        [along_z(up[:cut], 1, f"gather{half}"), along_z(down[cut:], -1, f"gather{half}")], axis=0
    )
    return held


def reduce_ring(parts, late):
    rings = lax.axis_size("rep") // 4
    half = rings // 2
    cut = parts[0].shape[0] // 2
    far = parts[half].astype(jnp.bfloat16)
    up, down = lax.optimization_barrier(
        (along_z(far[:cut], 1, f"reduce{half}"), along_z(far[cut:], -1, f"reduce{half}"))
    )
    up = jnp.concatenate([up, jnp.zeros_like(down)], axis=0)
    down = jnp.concatenate([jnp.zeros_like(up[:cut]), down], axis=0)
    for step in range(half - 1, 0, -1):
        up = (parts[step] + up.astype(jnp.float32)).astype(jnp.bfloat16)
        down = (parts[rings - step] + down.astype(jnp.float32)).astype(jnp.bfloat16)
        if step == 1:
            up, down, late = lax.optimization_barrier((up, down, late))
        up, down = lax.optimization_barrier(
            (along_z(up, 1, f"reduce{step}"), along_z(down, -1, f"reduce{step}"))
        )
    return parts[0] + up.astype(jnp.float32) + down.astype(jnp.float32), late


def local_slots(route_ids, experts):
    count = route_ids.shape[0]
    flat = route_ids.reshape(count * 2)
    onehot = (flat[:, None] == jnp.arange(experts, dtype=jnp.int32)[None, :]).astype(jnp.int32)
    before = jnp.cumsum(onehot, axis=0) - onehot
    return jnp.sum(before * onehot, axis=1).reshape(count, 2)


def body(
    route_ids,
    route_weight,
    input_float,
    input_quant,
    keep_mask,
    grad_mixed,
    gate_weight,
    up_weight,
    down_base,
    down_round,
    down_step,
):
    experts = lax.axis_size("expert")
    rings = lax.axis_size("rep") // 4
    here = lax.axis_index("rep")
    at_core, at_z = (here & 1, here >> 2)
    count = route_ids.shape[0]
    capacity = count // 2
    slot = local_slots(route_ids, experts)
    target = route_ids * capacity + slot
    columns = jnp.arange(experts * capacity, dtype=jnp.int32)
    first = (target[:, 0:1] == columns[None, :]).astype(jnp.float32)
    second = (target[:, 1:2] == columns[None, :]).astype(jnp.float32)
    placing = (first + second).astype(jnp.bfloat16)
    weighting = route_weight[:, 0:1] * first + route_weight[:, 1:2] * second
    x_in = jnp.where(keep_mask == 1, input_quant, input_float)
    all_grad = gather_tokens(grad_mixed)
    send_rows = lax.dot_general(
        placing, x_in, (((0,), (0,)), ((), ())), preferred_element_type=jnp.float32
    ).astype(jnp.bfloat16)
    spread = 2 * experts * count
    group = (here >> 1 & 1) * experts + lax.axis_index("expert")
    token = group * count + jnp.arange(count, dtype=jnp.int32)
    spot = (token[:, None] == jnp.arange(spread, dtype=jnp.int32)[None, :]).astype(jnp.float32)
    share = jnp.sum(jnp.swapaxes(weighting, 0, 1)[:, :, None] * spot[None], axis=1)
    high = lax.reduce_precision(share, 8, 7)
    low = (share - high).astype(jnp.bfloat16)
    send_rows = jnp.concatenate([send_rows, high.astype(jnp.bfloat16), low], axis=1)
    own_rows = exchange(jnp.concatenate([send_rows, send_rows], axis=0))
    width = x_in.shape[1]
    units = gate_weight.shape[2]
    w_gate = jnp.swapaxes(gate_weight[0], 0, 1)
    w_up = jnp.swapaxes(up_weight[0], 0, 1)
    soft = jax.nn.sigmoid(down_round[0].astype(jnp.float32))
    step_row = down_step[0][None, :]
    quant_down = (down_base[0].astype(jnp.float32) + step_row * soft).astype(jnp.bfloat16)
    quant_down, slope = lax.optimization_barrier((quant_down, step_row * soft * (1.0 - soft)))
    beside = ((0, 0), (0, 2 * spread))
    w_gate = jnp.pad(jnp.concatenate([w_gate, swap_cores(w_gate)], axis=0), beside)
    w_up = jnp.pad(jnp.concatenate([w_up, swap_cores(w_up)], axis=0), beside)
    quant_down = jnp.concatenate([quant_down, swap_cores(quant_down)], axis=0)
    size = own_rows.shape[0]
    held = gather_ring(own_rows)

    def hidden_of(which):
        x = jnp.concatenate([held[k] for k in which], axis=0)
        dims = (((1,), (1,)), ((), ()))
        gate = lax.dot_general(x, w_gate, dims, preferred_element_type=jnp.float32)
        up = lax.dot_general(x, w_up, dims, preferred_element_type=jnp.float32)
        return (jax.nn.silu(gate) * up).astype(jnp.bfloat16)

    half = rings // 2
    near = [k % rings for k in range(-(half - 2), half - 1)]
    hidden, part = ({}, {})
    for which in ([half, half - 1, half + 1], near):
        block = hidden_of(which)
        for i, k in enumerate(which):
            hidden[k] = block[size * i : size * (i + 1)]
    block = jnp.concatenate([hidden[k] for k in [half, half - 1, half + 1] + near], axis=0)
    out = jnp.dot(block, quant_down, preferred_element_type=jnp.float32)
    for i, k in enumerate([half, half - 1, half + 1] + near):
        part[k] = out[size * i : size * (i + 1)]
    summed, all_grad = reduce_ring(part, all_grad)
    summed = summed.astype(jnp.bfloat16)
    placed = jnp.zeros((rings, size, 2 * spread + 2 * units), jnp.bfloat16)
    for k in range(rings):
        block = jnp.concatenate([held[k][:, width:], hidden[k]], axis=1)[None]
        placed = lax.dynamic_update_slice_in_dim(placed, block, (at_z + k) & (rings - 1), axis=0)
    tokens = lax.dot_general(
        placed[..., : 2 * spread],
        placed[..., 2 * spread :],
        (((1,), (1,)), ((0,), (0,))),
        preferred_element_type=jnp.float32,
    )
    tokens = (tokens[:, :spread] + tokens[:, spread:]).astype(jnp.bfloat16)
    tokens = tokens.reshape(rings, 2 * experts, count, 2 * units)
    ours, other = (tokens[..., :units], swap_cores(tokens[..., units:]))
    full = jnp.where(
        at_core == 0, jnp.stack([ours, other], axis=2), jnp.stack([other, ours], axis=2)
    ).reshape(2 * rings * spread, units)
    grad_w = lax.dot_general(
        full, all_grad, (((0,), (0,)), ((), ())), preferred_element_type=jnp.float32
    )
    round_grad = (grad_w * slope)[None]
    summed, round_grad = lax.optimization_barrier((summed, round_grad))
    returned = exchange(summed)
    mixed = jnp.dot(
        jnp.concatenate([weighting, weighting], axis=1),
        returned.astype(jnp.float32),
        precision=lax.Precision.HIGHEST,
        preferred_element_type=jnp.float32,
    ).astype(jnp.bfloat16)
    return (mixed, round_grad)


def solution(mesh):
    return jax.shard_map(
        body,
        mesh=mesh,
        in_specs=(
            P(("expert", "rep"), None),
            P(("expert", "rep"), None),
            P(("expert", "rep"), None),
            P(("expert", "rep"), None),
            P(("expert", "rep"), None),
            P(("expert", "rep"), None),
            P("expert", None, "rep"),
            P("expert", None, "rep"),
            P("expert", "rep", None),
            P("expert", "rep", None),
            P("expert", None),
        ),
        out_specs=(P(("expert", "rep"), None), P("expert", "rep", None)),
        check_vma=False,
    )
```

```python
import jax
import jax.numpy as jnp
from jax import lax
from jax.sharding import PartitionSpec as P


BOTH = ("expert", "rep")


def swap_cores(a):
    n = lax.axis_size("rep")
    return lax.ppermute(a, "rep", [(r, r ^ 1) for r in range(n)])


def along_z(a, sign, name):
    n = lax.axis_size("rep")
    with jax.named_scope(name + ("_up" if sign > 0 else "_down")):
        return lax.ppermute(a, "rep", [(r, (r + 4 * sign) % n) for r in range(n)])


def exchange(a):
    experts, n = (lax.axis_size("expert"), lax.axis_size("rep"))
    groups = [
        [e * n + 4 * z + 2 * y + c for y in range(2) for e in range(experts)]
        for z in range(n // 4)
        for c in range(2)
    ]
    return lax.all_to_all(
        a, BOTH, split_axis=0, concat_axis=0, tiled=True, axis_index_groups=groups
    )


def along_column(a):
    n = lax.axis_size("rep")
    groups = [[4 * z + r for z in range(n // 4)] for r in range(4)]
    return lax.all_to_all(
        jnp.tile(a, (n // 4, 1)),
        "rep",
        split_axis=0,
        concat_axis=0,
        tiled=True,
        axis_index_groups=groups,
    )


def over_plane(a):
    experts, n = (lax.axis_size("expert"), lax.axis_size("rep"))
    groups = [
        [e * n + 4 * z + 2 * y + c for y in range(2) for e in range(experts) for c in range(2)]
        for z in range(n // 4)
    ]
    return lax.all_gather(a, BOTH, axis=0, tiled=True, axis_index_groups=groups)


def gather_ring(rows):
    rings = lax.axis_size("rep") // 4
    half = rings // 2
    cut = rows.shape[0] // 2
    held = {0: rows}
    up = down = rows
    for step in range(1, half):
        up, down = lax.optimization_barrier(
            (along_z(up, 1, f"gather{step}"), along_z(down, -1, f"gather{step}"))
        )
        held[rings - step], held[step] = (up, down)
    held[half] = jnp.concatenate(
        [along_z(up[:cut], 1, f"gather{half}"), along_z(down[cut:], -1, f"gather{half}")], axis=0
    )
    return held


def reduce_ring(parts, late):
    rings = lax.axis_size("rep") // 4
    half = rings // 2
    cut = parts[0].shape[0] // 2
    far = parts[half].astype(jnp.bfloat16)
    up, down = lax.optimization_barrier(
        (along_z(far[:cut], 1, f"reduce{half}"), along_z(far[cut:], -1, f"reduce{half}"))
    )
    up = jnp.concatenate([up, jnp.zeros_like(down)], axis=0)
    down = jnp.concatenate([jnp.zeros_like(up[:cut]), down], axis=0)
    for step in range(half - 1, 0, -1):
        up = (parts[step] + up.astype(jnp.float32)).astype(jnp.bfloat16)
        down = (parts[rings - step] + down.astype(jnp.float32)).astype(jnp.bfloat16)
        if step == 1:
            up, down, late = lax.optimization_barrier((up, down, late))
        up, down = lax.optimization_barrier(
            (along_z(up, 1, f"reduce{step}"), along_z(down, -1, f"reduce{step}"))
        )
    return parts[0] + up.astype(jnp.float32) + down.astype(jnp.float32), late


def local_slots(route_ids, experts):
    count = route_ids.shape[0]
    flat = route_ids.reshape(count * 2)
    onehot = (flat[:, None] == jnp.arange(experts, dtype=jnp.int32)[None, :]).astype(jnp.int32)
    before = jnp.cumsum(onehot, axis=0) - onehot
    return jnp.sum(before * onehot, axis=1).reshape(count, 2)


def body(
    route_ids,
    route_weight,
    input_float,
    input_quant,
    keep_mask,
    grad_mixed,
    gate_weight,
    up_weight,
    down_base,
    down_round,
    down_step,
):
    experts = lax.axis_size("expert")
    rings = lax.axis_size("rep") // 4
    here = lax.axis_index("rep")
    at_core, at_z = (here & 1, here >> 2)
    count = route_ids.shape[0]
    capacity = count // 2
    slot = local_slots(route_ids, experts)
    target = route_ids * capacity + slot
    columns = jnp.arange(experts * capacity, dtype=jnp.int32)
    first = (target[:, 0:1] == columns[None, :]).astype(jnp.float32)
    second = (target[:, 1:2] == columns[None, :]).astype(jnp.float32)
    placing = (first + second).astype(jnp.bfloat16)
    weighting = route_weight[:, 0:1] * first + route_weight[:, 1:2] * second
    x_in = jnp.where(keep_mask == 1, input_quant, input_float)
    column = along_column(grad_mixed)
    send_rows = lax.dot_general(
        placing, x_in, (((0,), (0,)), ((), ())), preferred_element_type=jnp.float32
    ).astype(jnp.bfloat16)
    spread = 2 * experts * count
    group = (here >> 1 & 1) * experts + lax.axis_index("expert")
    token = group * count + jnp.arange(count, dtype=jnp.int32)
    spot = (token[:, None] == jnp.arange(spread, dtype=jnp.int32)[None, :]).astype(jnp.float32)
    share = jnp.sum(jnp.swapaxes(weighting, 0, 1)[:, :, None] * spot[None], axis=1)
    send_rows = jnp.concatenate([send_rows, share.astype(jnp.bfloat16)], axis=1)
    send_rows, column = lax.optimization_barrier((send_rows, column))
    all_grad = over_plane(column)
    own_rows = exchange(jnp.concatenate([send_rows, send_rows], axis=0))
    width = x_in.shape[1]
    units = gate_weight.shape[2]
    w_gate = jnp.swapaxes(gate_weight[0], 0, 1)
    w_up = jnp.swapaxes(up_weight[0], 0, 1)
    soft = jax.nn.sigmoid(down_round[0].astype(jnp.float32))
    step_row = down_step[0][None, :]
    quant_down = (down_base[0].astype(jnp.float32) + step_row * soft).astype(jnp.bfloat16)
    quant_down, slope = lax.optimization_barrier((quant_down, step_row * soft * (1.0 - soft)))
    beside = ((0, 0), (0, spread))
    w_gate = jnp.pad(jnp.concatenate([w_gate, swap_cores(w_gate)], axis=0), beside)
    w_up = jnp.pad(jnp.concatenate([w_up, swap_cores(w_up)], axis=0), beside)
    quant_down = jnp.concatenate([quant_down, swap_cores(quant_down)], axis=0)
    size = own_rows.shape[0]
    held = gather_ring(own_rows)

    def hidden_of(which):
        x = jnp.concatenate([held[k] for k in which], axis=0)
        dims = (((1,), (1,)), ((), ()))
        gate = lax.dot_general(x, w_gate, dims, preferred_element_type=jnp.float32)
        up = lax.dot_general(x, w_up, dims, preferred_element_type=jnp.float32)
        return (jax.nn.silu(gate) * up).astype(jnp.bfloat16)

    half = rings // 2
    near = [k % rings for k in range(-(half - 2), half - 1)]
    hidden, part = ({}, {})
    for which in ([half, half - 1, half + 1], near):
        block = hidden_of(which)
        for i, k in enumerate(which):
            hidden[k] = block[size * i : size * (i + 1)]
    block = jnp.concatenate([hidden[k] for k in [half, half - 1, half + 1] + near], axis=0)
    out = jnp.dot(block, quant_down, preferred_element_type=jnp.float32)
    for i, k in enumerate([half, half - 1, half + 1] + near):
        part[k] = out[size * i : size * (i + 1)]
    summed, all_grad = reduce_ring(part, all_grad)
    summed = summed.astype(jnp.bfloat16)
    placed = jnp.zeros((rings, size, spread + 2 * units), jnp.bfloat16)
    for k in range(rings):
        block = jnp.concatenate([held[k][:, width:], hidden[k]], axis=1)[None]
        placed = lax.dynamic_update_slice_in_dim(placed, block, (at_z + k) & (rings - 1), axis=0)
    tokens = lax.dot_general(
        placed[..., :spread],
        placed[..., spread:],
        (((1,), (1,)), ((0,), (0,))),
        preferred_element_type=jnp.float32,
    )
    tokens = tokens.astype(jnp.bfloat16).reshape(rings, 2 * experts, count, 2 * units)
    ours, other = (tokens[..., :units], swap_cores(tokens[..., units:]))
    full = jnp.where(
        at_core == 0, jnp.stack([ours, other], axis=2), jnp.stack([other, ours], axis=2)
    )
    full = jnp.transpose(full, (1, 2, 0, 3, 4)).reshape(2 * rings * spread, units)
    grad_w = lax.dot_general(
        full, all_grad, (((0,), (0,)), ((), ())), preferred_element_type=jnp.float32
    )
    round_grad = (grad_w * slope)[None]
    summed, round_grad = lax.optimization_barrier((summed, round_grad))
    returned = exchange(summed)
    mixed = jnp.dot(
        jnp.concatenate([weighting, weighting], axis=1),
        returned.astype(jnp.float32),
        precision=lax.Precision.HIGHEST,
        preferred_element_type=jnp.float32,
    ).astype(jnp.bfloat16)
    return (mixed, round_grad)


def solution(mesh):
    return jax.shard_map(
        body,
        mesh=mesh,
        in_specs=(
            P(("expert", "rep"), None),
            P(("expert", "rep"), None),
            P(("expert", "rep"), None),
            P(("expert", "rep"), None),
            P(("expert", "rep"), None),
            P(("expert", "rep"), None),
            P("expert", None, "rep"),
            P("expert", None, "rep"),
            P("expert", "rep", None),
            P("expert", "rep", None),
            P("expert", None),
        ),
        out_specs=(P(("expert", "rep"), None), P("expert", "rep", None)),
        check_vma=False,
    )
```
